32 devices in a mesh: ga: 2 (over x), aa: 8 (over z, y), ba: 2 (over core).
Axes of the slice: x: 2, y: 2, z: 4, core: 2. Of those that a mesh axis runs over, the one named last changes fastest.
Arguments:
- images: bfloat16 [2048, 12, 4096], P(('ga', 'aa', 'ba')), parts along dimension 0, may hold values from -6 to 6
- key_projection: bfloat16 [4096, 512], replicated, may hold values from -0.09375 to 0.09375
- value_projection: bfloat16 [4096, 512], replicated, may hold values from -0.09375 to 0.09375
- key_norm_gain: float32 [128], replicated, may hold values from 0.1 to 1.9
- hidden: bfloat16 [2048, 4096], P(('ga', 'aa'), 'ba'), parts along dimension 0, may hold values from -6 to 6
- shared_query_base: bfloat16 [2048, 2048], P(('ga', 'aa'), 'ba'), parts along dimension 0, may hold values from -220 to 220
- adapter_down_matrix: bfloat16 [8, 4096, 16], P('aa'), may hold values from -0.09375 to 0.09375
- adapter_up_matrix: bfloat16 [8, 16, 2048], P('aa'), may hold values from -1.5 to 1.5
- tenant_adapter_index: int32 [2048, 1], P(('ga', 'aa')), parts along dimension 0, may hold values from 0 to 7; in each aligned block of 128 rows (0 to 127, 128 to 255, ...) at most 32 rows name the same one
- used_tile_count: int32 [2048], P(('ga', 'aa', 'ba')), parts along dimension 0, may hold values from 1 to 4
Outputs:
- attended: bfloat16 [2048, 2048], P(('ga', 'aa', 'ba')), parts along dimension 0
The draws below stay inside these ranges and needn't reach their ends.
There are 2 independent parts, one for each index of `ga`. The reference program is written for one: setup_inputs(seed, part) draws one part's arguments, and reference() takes and returns one part's arrays. A program takes and returns all parts, laid end to end along the dimension named above; an argument that names none is the same for every part. Nothing has to cross between parts.
Inputs may be any that keep to these rules, and one draw needn't show every extreme that they name: `tenant_adapter_index`: among the 128 requests of one index of aa (aligned blocks) no adapter is named more than 32 times.
All inputs are finite; a program needn't handle non-finite values.
Results may differ from the reference program's by a relative error of at most 0.012.
The reference program's roundings to bfloat16 on the way count: a program that leaves them out, or rounds other values in their place, can miss the bound.
Values may be sent and summed in bfloat16 or wider, within the bound.
A program may use at most 128 MiB of HBM per device.

```python
import math
import jax
import jax.numpy as jnp
import numpy as np
from jax import lax

MODEL_WIDTH = 4096
HEAD_WIDTH = 128
QUERY_HEADS = 16
KEY_VALUE_HEADS = 4
ADAPTER_RANK = 16
TILE_SLOTS = 4
TILE_TOKENS = 3
REQ_DEV = 128
REQUEST_TOTAL = 1024
ADAPTER_TOTAL = 8
MOST = 32
QUERY_WIDTH = 2048
KVW = 512


def draw_shared_query_base(key, part):
    key_values = jax.random.fold_in(jax.random.fold_in(key, 17), 0)
    normal_part = jnp.clip(jax.random.normal(key_values, (REQUEST_TOTAL, QUERY_WIDTH), jnp.float32), -6.0, 6.0)
    return normal_part.astype(jnp.bfloat16)


def place_ends(entries, own_key, smallest, largest):
    spot = [jax.random.randint(jax.random.fold_in(own_key, axis), (), 0, length) for axis, length in enumerate(entries.shape)]
    longest = entries.shape.index(max(entries.shape))
    next_to = spot[:longest] + [(spot[longest] + 1) % entries.shape[longest]] + spot[longest + 1:]
    return entries.at[tuple(spot)].set(smallest).at[tuple(next_to)].set(largest)


def level_of(own_key, extent, cuts, smallest, high):
    level = 1.0
    for dim, shards_of in cuts:
        steps = jax.random.uniform(jax.random.fold_in(jax.random.fold_in(own_key, 6), dim), (shards_of,), jnp.float32, smallest / len(cuts), high / len(cuts))
        level = level * jnp.repeat(jnp.exp(steps), extent[dim] // shards_of).reshape((-1,) + (1,) * (len(extent) - 1 - dim))
    return level


def assign_block(stream_key, own, number, rows, count, top, most, slope):
    order = jax.random.permutation(stream_key, count)
    heavy_load, common = shares(count, rows * top, most, slope, True), shares(count, rows * top, most, slope, False)
    places = jnp.arange(count)

    def named(sizes, offset_by):
        used = int((sizes > 0).sum())
        fixed = max(1, used // 4)
        passed = fixed + (places - fixed + offset_by * (used - fixed)) % max(1, count - fixed)
        return jnp.zeros((count,), jnp.int32).at[order[jnp.where(places < fixed, places, passed)]].set(jnp.asarray(sizes, jnp.int32))

    sizes = jnp.where(number % 4 == 0, named(heavy_load, number // 4), named(common, number - number // 4 - 1))
    mixed = jax.random.permutation(jax.random.fold_in(own, 3), count)
    donor, receiver = mixed[0:count // 2 * 2:2], mixed[1:count // 2 * 2:2]
    room = jnp.minimum(sizes[donor] - 1, most - sizes[receiver]) // 2
    room = jnp.where((donor == order[0]) | (receiver == order[0]) | (sizes[receiver] == 0), 0, jnp.maximum(room, 0))
    passed = jax.random.randint(jax.random.fold_in(own, 4), (count // 2,), 0, 1 << 20) % (room + 1)
    sizes = sizes.at[donor].add(-passed).at[receiver].add(passed)
    members = jnp.searchsorted(jnp.cumsum(sizes), jnp.arange(rows * top), side="right").astype(jnp.int32)
    table = members.reshape(top, rows).T
    table = table[jax.random.permutation(jax.random.fold_in(own, 1), rows)]
    offset_by = jax.random.randint(jax.random.fold_in(own, 2), (rows, 1), 0, top)
    return jnp.take_along_axis(table, (jnp.arange(top)[None, :] + offset_by) % top, axis=1)


def shares(amount, total, most, slope, full):
    weights = [(1 << 20) // math.isqrt(standing ** slope) + 1 for standing in range(1, amount + 1)]
    largest = most if full else min(most, max(-(-total // amount), total * weights[0] // sum(weights)))
    least = 1 if total - largest >= amount - 1 else 0
    holding, spare = [largest] + [least] * (amount - 1), total - largest - least * (amount - 1)
    while spare > 0:
        candidates = [i for i in range(1, amount) if holding[i] < largest] or [i for i in range(1, amount) if holding[i] < most]
        mass, remaining = sum([weights[i] for i in candidates]), spare
        for i in candidates:
            addition = min(most - holding[i], max(1, remaining * weights[i] // mass), spare)
            holding[i] = holding[i] + addition
            spare = spare - addition
    return np.array(holding)


def bell_draw(key, shape, spread, bound, pieces=(), kind=jnp.bfloat16):
    entries = spread * jax.random.normal(key, shape, jnp.float32)
    if pieces:
        entries = entries * level_of(key, shape, pieces, -0.22, 0.18)
    return jnp.clip(entries, -bound, bound).astype(kind)


def setup_inputs(seed: int = 0, part: int = 0) -> dict:
    keys = jax.random.split(jax.random.key(seed), 11)
    own_keys = jax.random.split(jax.random.fold_in(keys[10], part), 11)
    images = bell_draw(own_keys[0], (REQUEST_TOTAL, TILE_SLOTS * TILE_TOKENS, MODEL_WIDTH), 1.0, 6.0, ((0, 16),))
    key_projection = bell_draw(keys[1], (MODEL_WIDTH, KVW), MODEL_WIDTH ** -0.5, 0.09375)
    value_projection = bell_draw(keys[2], (MODEL_WIDTH, KVW), MODEL_WIDTH ** -0.5, 0.09375)
    key_norm_gain = jnp.clip(1.0 + 0.18 * jax.random.normal(keys[3], (HEAD_WIDTH,), jnp.float32), 0.1, 1.9)
    hidden = bell_draw(own_keys[4], (REQUEST_TOTAL, MODEL_WIDTH), 1.0, 6.0, ((0, 8), (1, 2)))
    shared_query_base = draw_shared_query_base(jax.random.fold_in(jax.random.fold_in(keys[10], part), 71), part)
    adapter_down_matrix = bell_draw(keys[6], (ADAPTER_TOTAL, MODEL_WIDTH, ADAPTER_RANK), MODEL_WIDTH ** -0.5, 0.09375, ((0, 8),))
    adapter_up_matrix = bell_draw(keys[7], (ADAPTER_TOTAL, ADAPTER_RANK, QUERY_WIDTH), ADAPTER_RANK ** -0.5, 1.5, ((0, 8),))
    tenant_adapter_index_keys = jax.random.split(jax.random.fold_in(own_keys[8], 1), REQUEST_TOTAL // REQ_DEV)
    tenant_adapter_index_turns = jax.random.permutation(jax.random.fold_in(own_keys[8], 3), REQUEST_TOTAL // REQ_DEV)
    tenant_adapter_index = jax.vmap(lambda own, number: assign_block(jax.random.fold_in(own_keys[8], 2), own, number, REQ_DEV, ADAPTER_TOTAL, 1, MOST, 2))(tenant_adapter_index_keys, tenant_adapter_index_turns).reshape((REQUEST_TOTAL, 1))
    used_tile_count = place_ends(jax.random.randint(own_keys[9], (REQUEST_TOTAL,), 1, TILE_SLOTS + 1), jax.random.fold_in(own_keys[9], 1), 1, TILE_SLOTS).astype(jnp.int32)
    return dict(images=images, key_projection=key_projection, value_projection=value_projection, key_norm_gain=key_norm_gain, hidden=hidden, shared_query_base=shared_query_base, adapter_down_matrix=adapter_down_matrix, adapter_up_matrix=adapter_up_matrix, tenant_adapter_index=tenant_adapter_index, used_tile_count=used_tile_count)


def reference(images, key_projection, value_projection, key_norm_gain, hidden, shared_query_base, adapter_down_matrix, adapter_up_matrix, tenant_adapter_index, used_tile_count):
    flattened_rows = images.reshape(REQUEST_TOTAL * TILE_SLOTS * TILE_TOKENS, MODEL_WIDTH)
    unnormed_keys = jnp.dot(flattened_rows, key_projection, preferred_element_type=jnp.float32).reshape(REQUEST_TOTAL, TILE_SLOTS * TILE_TOKENS, KEY_VALUE_HEADS, HEAD_WIDTH)
    key_scale = lax.rsqrt(lax.optimization_barrier(jnp.mean(unnormed_keys * unnormed_keys, axis=-1, keepdims=True)) + 1e-06)
    keys_all = (unnormed_keys * key_scale * key_norm_gain.astype(jnp.float32)).astype(jnp.bfloat16)
    gathered_values = jnp.dot(flattened_rows, value_projection, preferred_element_type=jnp.float32).astype(jnp.bfloat16)
    gathered_values = gathered_values.reshape(REQUEST_TOTAL, TILE_SLOTS * TILE_TOKENS, KEY_VALUE_HEADS, HEAD_WIDTH)
    owner_hot = (tenant_adapter_index[:, 0:1] == jnp.arange(ADAPTER_TOTAL, dtype=jnp.int32)[None, :]).astype(jnp.float32)
    widened_down_matrix = jnp.transpose(adapter_down_matrix, (1, 0, 2)).reshape(MODEL_WIDTH, ADAPTER_TOTAL * ADAPTER_RANK)
    low_all = jnp.dot(hidden, widened_down_matrix, preferred_element_type=jnp.float32).reshape(REQUEST_TOTAL, ADAPTER_TOTAL, ADAPTER_RANK)
    reduced_rank_part = lax.optimization_barrier(jnp.sum(low_all * owner_hot[:, :, None], axis=1))
    widened_reduced_part = owner_hot.astype(jnp.bfloat16)[:, :, None] * reduced_rank_part.astype(jnp.bfloat16)[:, None, :]
    adapter_query_delta = jnp.dot(widened_reduced_part.reshape(REQUEST_TOTAL, ADAPTER_TOTAL * ADAPTER_RANK), adapter_up_matrix.reshape(ADAPTER_TOTAL * ADAPTER_RANK, QUERY_WIDTH), preferred_element_type=jnp.float32).astype(jnp.bfloat16)
    query_rows = (shared_query_base.astype(jnp.float32) + adapter_query_delta.astype(jnp.float32)).astype(jnp.bfloat16)
    query_group_width = QUERY_HEADS // KEY_VALUE_HEADS
    query_four_axes = query_rows.reshape(REQUEST_TOTAL, KEY_VALUE_HEADS, query_group_width, HEAD_WIDTH).astype(jnp.float32)
    scores = jnp.einsum('rkgd,rjkd->rkgj', query_four_axes, keys_all.astype(jnp.float32)) / math.sqrt(HEAD_WIDTH)
    position = jnp.arange(TILE_SLOTS * TILE_TOKENS, dtype=jnp.int32) // TILE_TOKENS
    valid_rows = position[None, :] < used_tile_count[:, None]
    key_mask = valid_rows[:, None, None, :]
    scores = jnp.where(key_mask, scores, -jnp.inf)
    score_peak = lax.optimization_barrier(jnp.max(scores, axis=-1, keepdims=True))
    weights = jnp.exp(scores - score_peak)
    weight_total = lax.optimization_barrier(jnp.sum(weights, axis=-1))
    rounded = lax.optimization_barrier(weights.astype(jnp.bfloat16)).astype(jnp.float32)
    weighted = jnp.einsum('rkgj,rjkd->rkgd', rounded, gathered_values.astype(jnp.float32))
    attended = (weighted / weight_total[..., None]).reshape(REQUEST_TOTAL, QUERY_WIDTH).astype(jnp.bfloat16)
    return attended
```

```python
import functools
import math

import jax
import jax.numpy as jnp
from jax import lax
from jax.experimental import pallas as pl
from jax.experimental.pallas import tpu as pltpu
from jax.sharding import PartitionSpec as P

TILE_TOKENS = 3
REQUEST_BLOCK = 16
CHUNKS = 8
MESH = pl.DeviceIdType.MESH
NT = (((1,), (1,)), ((), ()))


def grid_of(count):
    inner = max(d for d in range(1, count + 1) if count % d == 0 and d * d <= count)
    return count // inner, inner


def kernel(
    outer, inner, images, wk_hbm, wv_hbm, hidden, base, down, up, gain, ids, used, out,
    img, wk, wv, acc, keys, vals, all_down, all_up, hid, bas,
    in_sem, own_sem, zs, zr, ys, yr, ps, pr, xs, xr,
):
    chunks, rows, depth = img.shape
    _, here, half_model = hid.shape
    half_query = bas.shape[2]
    rank = down.shape[0]
    head = gain.shape[1]
    width = wk.shape[2]
    heads_kv = width // head
    group = 2 * half_query // width
    tokens = rows // here

    me = lax.axis_index("aa")
    side = lax.axis_index("ba")
    other = 1 - side
    z, y = me // inner, lax.rem(me, inner)

    def at_z(d):
        return {"aa": lax.rem(z + d, outer) * inner + y}

    def at_y(e):
        return {"aa": z * inner + lax.rem(y + e, inner)}

    partner = {"ba": other}

    loads = []
    for c in range(chunks):
        cols = pl.ds(c * depth, depth)
        loads.append([
            pltpu.make_async_copy(images.at[:, cols], img.at[c], in_sem.at[c, 0]),
            pltpu.make_async_copy(wk_hbm.at[cols], wk.at[c], in_sem.at[c, 1]),
            pltpu.make_async_copy(wv_hbm.at[cols], wv.at[c], in_sem.at[c, 2]),
        ])
    for copy in loads[0]:
        copy.start()

    def halves(ref, s, size):
        return ref.at[:, pl.ds(pl.multiple_of(s * size, 128), size)]

    mine = pl.ds(pl.multiple_of(side * here, here), here)
    theirs = pl.ds(pl.multiple_of(other * here, here), here)

    barrier = pltpu.get_barrier_semaphore()
    greeted = [at_z(d) for d in range(1, outer)] + [at_y(e) for e in range(1, inner)] + [partner]
    for device in greeted:
        pl.semaphore_signal(barrier, inc=1, device_id=device, device_id_type=MESH)
    for copies in loads[1:]:
        for copy in copies:
            copy.start()
    local = [
        pltpu.make_async_copy(hidden.at[mine], hid.at[side], own_sem.at[0]),
        pltpu.make_async_copy(base.at[mine], bas.at[side], own_sem.at[1]),
    ]
    own_rows = pl.ds(pl.multiple_of(me * rank, rank), rank)
    for s in range(2):
        local.append(pltpu.make_async_copy(
            halves(down, s, half_model), all_down.at[s, own_rows], own_sem.at[2 + s]))
        local.append(pltpu.make_async_copy(
            halves(up, s, half_query), all_up.at[s, own_rows], own_sem.at[4 + s]))
    pl.semaphore_wait(barrier, len(greeted))

    def block_rows(d, e):
        b = lax.rem(z + (outer - d), outer) * inner + lax.rem(y + (inner - e), inner)
        return pl.ds(pl.multiple_of(b * rank, rank), rank)

    def send(d, e, device, ssem, rsem, slot):
        r = block_rows(d, e)
        if d == 0 and e == 0:
            sources = (halves(down, side, half_model), halves(up, side, half_query))
        else:
            sources = (all_down.at[side, r], all_up.at[side, r])
        targets = (all_down.at[side, r], all_up.at[side, r])
        made = []
        for i in range(2):
            made.append(pltpu.make_async_remote_copy(
                src_ref=sources[i], dst_ref=targets[i],
                send_sem=ssem.at[slot, i], recv_sem=rsem.at[slot, i],
                device_id=device, device_id_type=MESH))
        for copy in made:
            copy.start()
        return made

    near = sorted(range(1, outer), key=lambda d: min(d, outer - d))
    z_copies = {d: send(0, 0, at_z(d), zs, zr, d) for d in near}
    y_copies = {(0, e): send(0, 0, at_y(e), ys, yr, e) for e in range(1, inner)}
    swaps = []
    for i, (src, dst) in enumerate(((hidden, hid), (base, bas))):
        swaps.append(pltpu.make_async_remote_copy(
            src_ref=src.at[theirs], dst_ref=dst.at[side],
            send_sem=xs.at[i], recv_sem=xr.at[i], device_id=partner, device_id_type=MESH))
    for copy in swaps:
        copy.start()
    for copy in local:
        copy.start()
    p_copies = []

    def arrived(copies):
        for copy in copies:
            copy.wait_recv()

    def pass_z(d):
        arrived(z_copies[d])
        for e in range(1, inner):
            y_copies[d, e] = send(d, 0, at_y(e), ys, yr, d * inner + e)
        p_copies.extend(send(d, 0, partner, ps, pr, d * inner))

    def pass_y(d):
        for e in range(1, inner):
            arrived(y_copies[d, e])
            p_copies.extend(send(d, e, partner, ps, pr, d * inner + e))

    jobs = [functools.partial(pass_z, d) for d in near] + [
        functools.partial(pass_y, d) for d in [0] + near]
    first = chunks // 2
    for c in range(chunks):
        for copy in loads[c]:
            copy.wait()
        for part, w in enumerate((wk, wv)):
            cols = slice(part * width, (part + 1) * width)
            term = jnp.dot(img[c], w[c], preferred_element_type=jnp.float32)
            if c == 0:
                acc[:, cols] = term
            else:
                acc[:, cols] += term
        if c >= first and len(jobs) > outer:
            jobs.pop(0)()
    while len(jobs) > outer:
        jobs.pop(0)()

    g = gain[...]
    for k in range(heads_kv):
        cols = slice(k * head, (k + 1) * head)
        x = acc[:, cols]
        scale = lax.rsqrt(jnp.mean(x * x, axis=-1, keepdims=True) + 1e-06)
        keys[:, :, cols] = (x * scale * g).astype(jnp.bfloat16).reshape(tokens, here, head)
    vals[...] = acc[:, width:].astype(jnp.bfloat16).reshape(tokens, here, width)

    for job in jobs:
        job()
    for copy in local:
        copy.wait()
    arrived(swaps)
    arrived(p_copies)

    id_row = ids[...]
    requests = id_row.shape[1]
    row_at = lax.broadcasted_iota(jnp.int32, (here, requests), 0) + side * here
    col_at = lax.broadcasted_iota(jnp.int32, (here, requests), 1)
    id_col = jnp.sum(jnp.where(row_at == col_at, id_row, 0), axis=1, keepdims=True)
    low = lax.dot_general(hid[0], all_down[0], NT, preferred_element_type=jnp.float32)
    low += lax.dot_general(hid[1], all_down[1], NT, preferred_element_type=jnp.float32)
    lane = lax.broadcasted_iota(jnp.int32, low.shape, 1)
    owned = (lane >= id_col * rank) & (lane < id_col * rank + rank)
    low = jnp.where(owned, low, 0.0).astype(jnp.bfloat16)
    queries = []
    for s in range(2):
        delta = jnp.dot(low, all_up[s], preferred_element_type=jnp.float32).astype(jnp.bfloat16)
        queries.append(
            (bas[s].astype(jnp.float32) + delta.astype(jnp.float32)).astype(jnp.bfloat16))
    queries = jnp.concatenate(queries, axis=1)

    eye = lax.broadcasted_iota(jnp.int32, (here, here), 0) == lax.broadcasted_iota(
        jnp.int32, (here, here), 1)
    used_col = jnp.sum(jnp.where(eye, used[...], 0), axis=1, keepdims=True)
    nb = REQUEST_BLOCK
    shape = (group * nb, tokens * nb)
    r_at = lax.broadcasted_iota(jnp.int32, shape, 0)
    c_at = lax.broadcasted_iota(jnp.int32, shape, 1)
    same = (r_at & (nb - 1)) == (c_at & (nb - 1))
    for b in range(here // nb):
        rs = slice(b * nb, (b + 1) * nb)
        limit = jnp.concatenate([used_col[rs]] * group, axis=0) * (TILE_TOKENS * nb)
        mask = same & (c_at < limit)
        for k in range(heads_kv):
            cols = slice(k * head, (k + 1) * head)
            kb = keys[:, rs, cols].reshape(tokens * nb, head)
            vb = vals[:, rs, cols].reshape(tokens * nb, head)
            q = jnp.concatenate(
                [queries[rs, (k * group + i) * head:(k * group + i + 1) * head]
                 for i in range(group)], axis=0)
            scores = lax.dot_general(q, kb, NT, preferred_element_type=jnp.float32)
            scores = jnp.where(mask, scores * (1.0 / math.sqrt(head)), -1e30)
            peak = jnp.max(scores, axis=1, keepdims=True)
            weights = jnp.where(mask, jnp.exp(scores - peak), 0.0)
            total = jnp.sum(weights, axis=1, keepdims=True)
            mixed = jnp.dot(weights.astype(jnp.bfloat16), vb, preferred_element_type=jnp.float32)
            mixed = (mixed / total).astype(jnp.bfloat16)
            for i in range(group):
                out[rs, (k * group + i) * head:(k * group + i + 1) * head] = (
                    mixed[i * nb:(i + 1) * nb])

    for copies in list(z_copies.values()) + list(y_copies.values()) + [p_copies, swaps]:
        for copy in copies:
            copy.wait_send()


def on_device(
    images,
    key_projection,
    value_projection,
    key_norm_gain,
    hidden,
    shared_query_base,
    adapter_down_matrix,
    adapter_up_matrix,
    tenant_adapter_index,
    used_tile_count,
):
    here, tokens, model = images.shape
    rows = here * tokens
    width = key_projection.shape[1]
    half_model = hidden.shape[1]
    half_query = shared_query_base.shape[1]
    rank = adapter_down_matrix.shape[2]
    count = lax.axis_size("aa")
    outer, inner = grid_of(count)
    flat = jnp.transpose(images, (1, 0, 2)).reshape(rows, model)
    down = jnp.transpose(adapter_down_matrix[0])
    depth = model // CHUNKS
    bf16 = jnp.bfloat16
    hbm = pl.BlockSpec(memory_space=pl.ANY)
    vmem = pl.BlockSpec(memory_space=pltpu.VMEM)
    dma = pltpu.SemaphoreType.DMA
    return pl.pallas_call(
        functools.partial(kernel, outer, inner),
        out_shape=jax.ShapeDtypeStruct((here, 2 * half_query), bf16),
        in_specs=[hbm] * 7 + [vmem] * 3,
        out_specs=vmem,
        scratch_shapes=[
            pltpu.VMEM((CHUNKS, rows, depth), bf16),
            pltpu.VMEM((CHUNKS, depth, width), bf16),
            pltpu.VMEM((CHUNKS, depth, width), bf16),
            pltpu.VMEM((rows, 2 * width), jnp.float32),
            pltpu.VMEM((tokens, here, width), bf16),
            pltpu.VMEM((tokens, here, width), bf16),
            pltpu.VMEM((2, count * rank, half_model), bf16),
            pltpu.VMEM((2, count * rank, half_query), bf16),
            pltpu.VMEM((2, here, half_model), bf16),
            pltpu.VMEM((2, here, half_query), bf16),
            dma((CHUNKS, 3)),
            dma((6,)),
            dma((outer, 2)),
            dma((outer, 2)),
            dma((count, 2)),
            dma((count, 2)),
            dma((count, 2)),
            dma((count, 2)),
            dma((2,)),
            dma((2,)),
        ],
        compiler_params=pltpu.CompilerParams(
            collective_id=0, has_side_effects=True, vmem_limit_bytes=60 * 1024 * 1024
        ),
    )(
        flat,
        key_projection,
        value_projection,
        hidden,
        shared_query_base,
        down,
        adapter_up_matrix[0],
        key_norm_gain[None, :],
        tenant_adapter_index.reshape(1, -1),
        used_tile_count[None, :],
    )


def solution(mesh):
    placed = (
        P(("ga", "aa", "ba"), None, None),
        P(),
        P(),
        P(),
        P(("ga", "aa"), "ba"),
        P(("ga", "aa"), "ba"),
        P("aa", None, None),
        P("aa", None, None),
        P(("ga", "aa"), None),
        P(("ga", "aa", "ba")),
    )
    return jax.shard_map(
        on_device,
        mesh=mesh,
        in_specs=placed,
        out_specs=P(("ga", "aa", "ba"), None),
        check_vma=False,
    )
```

```python
import functools
import math

import jax
import jax.numpy as jnp
from jax import lax
from jax.experimental import pallas as pl
from jax.experimental.pallas import tpu as pltpu
from jax.sharding import PartitionSpec as P

TILE_TOKENS = 3
REQUEST_BLOCK = 16
CHUNKS = 8
MESH = pl.DeviceIdType.MESH
NT = (((1,), (1,)), ((), ()))


def grid_of(count):
    inner = max(d for d in range(1, count + 1) if count % d == 0 and d * d <= count)
    return count // inner, inner


def kernel(
    outer, inner, images, wk_hbm, wv_hbm, hidden, base, down, up, gain, ids, used, out,
    img, wk, wv, acc, keys, vals, all_down, all_up, hid, bas,
    in_sem, own_sem, zs, zr, ys, yr, ps, pr, xs, xr, gs, gr, hs, hr,
):
    chunks, rows, depth = img.shape
    _, here, half_model = hid.shape
    half_query = bas.shape[2]
    rank = down.shape[0]
    head = gain.shape[1]
    width = wk.shape[2]
    heads_kv = width // head
    group = 2 * half_query // width
    tokens = rows // here

    me = lax.axis_index("aa")
    side = lax.axis_index("ba")
    groups = lax.axis_size("ga")
    g_at = lax.axis_index("ga")
    quarter = half_model // groups
    other = 1 - side
    z, y = me // inner, lax.rem(me, inner)

    partner = {"ba": other}

    loads = []
    for c in range(chunks):
        cols = pl.ds(c * depth, depth)
        loads.append([
            pltpu.make_async_copy(images.at[:, cols], img.at[c], in_sem.at[c, 0]),
            pltpu.make_async_copy(wk_hbm.at[cols], wk.at[c], in_sem.at[c, 1]),
            pltpu.make_async_copy(wv_hbm.at[cols], wv.at[c], in_sem.at[c, 2]),
        ])
    for copy in loads[0]:
        copy.start()

    def halves(ref, s, size):
        start = s * size if isinstance(s, int) else pl.multiple_of(s * size, 128)
        return ref.at[:, pl.ds(start, size)]

    mine = pl.ds(pl.multiple_of(side * here, here), here)
    theirs = pl.ds(pl.multiple_of(other * here, here), here)

    local = [
        pltpu.make_async_copy(hidden.at[mine], hid.at[side], own_sem.at[0]),
        pltpu.make_async_copy(base.at[mine], bas.at[side], own_sem.at[1]),
    ]
    own_rows = pl.ds(pl.multiple_of(me * rank, rank), rank)
    for s in range(2):
        local.append(pltpu.make_async_copy(
            halves(up, s, half_query), all_up.at[s, own_rows], own_sem.at[2 + s]))
    for q in range(2 * groups):
        local.append(pltpu.make_async_copy(
            halves(down, q, quarter), all_down.at[q, own_rows], own_sem.at[4 + q]))

    def z_peer(d):
        if outer & (outer - 1):
            return lax.rem(z + d, outer)
        to, bit = z, 1
        while bit < outer:
            if d & bit:
                to = to + bit - 2 * bit * lax.rem(z // bit, 2)
            bit *= 2
        return to

    def z_from(d):
        return lax.rem(z + (outer - d), outer) if outer & (outer - 1) else z_peer(d)

    def block_rows(d, e):
        b = z_from(d) * inner + lax.rem(y + (inner - e), inner)
        return pl.ds(pl.multiple_of(b * rank, rank), rank)

    def y_peer(e):
        return {"aa": z * inner + lax.rem(y + e, inner)}

    def x_peer(f):
        return {"ga": lax.rem(g_at + f, groups)}

    def quarter_at(f):
        return side * groups + lax.rem(g_at + (groups - f), groups)

    started = []

    def push(src, dst, device, ssem, rsem):
        copy = pltpu.make_async_remote_copy(
            src_ref=src, dst_ref=dst, send_sem=ssem, recv_sem=rsem,
            device_id=device, device_id_type=MESH)
        copy.start()
        started.append(copy)
        return copy

    def piece(i, d, e, f=0):
        r = block_rows(d, e)
        return all_up.at[side, r] if i else all_down.at[quarter_at(f), r]

    own_piece = [
        down.at[:, pl.ds(pl.multiple_of(quarter_at(0) * quarter, 128), quarter)],
        halves(up, side, half_query),
    ]
    barrier = pltpu.get_barrier_semaphore()
    greeted = (
        [{"aa": z_peer(d) * inner + y} for d in range(1, outer)]
        + ([{"aa": z_from(d) * inner + y} for d in range(1, outer)] if outer & (outer - 1) else [])
        + [y_peer(e) for e in range(1, inner)]
        + [x_peer(f) for f in range(1, groups)]
        + [partner]
    )
    for device in greeted:
        pl.semaphore_signal(barrier, inc=1, device_id=device, device_id_type=MESH)
    for copies in loads[1:]:
        for copy in copies:
            copy.start()
    pl.semaphore_wait(barrier, len(greeted))

    got_z, got_y, got_x, got_p = {}, {}, {}, []
    turns = list(range(1, outer))
    for i in range(2):
        for d in turns:
            got_z[i, d] = push(
                own_piece[i], piece(i, 0, 0), {"aa": z_peer(d) * inner + y}, zs.at[d, i], zr.at[d, i])
        for e in range(1, inner):
            got_y[i, 0, e] = push(own_piece[i], piece(i, 0, 0), y_peer(e), ys.at[e, i], yr.at[e, i])
    for i, (src, dst) in enumerate(((hidden, hid), (base, bas))):
        got_p.append(push(src.at[theirs], dst.at[side], partner, xs.at[i], xr.at[i]))
    for copy in local:
        copy.start()

    def spread(i, d, e):
        slot = d * inner + e
        here_piece = piece(i, d, e)
        if i == 0:
            for f in range(1, groups):
                got_x[d, e, f] = push(
                    here_piece, here_piece, x_peer(f),
                    gs.at[slot * groups + f], gr.at[slot * groups + f])
        got_p.append(push(here_piece, here_piece, partner, ps.at[slot, i], pr.at[slot, i]))

    def pass_z(i, d):
        got_z[i, d].wait_recv()
        for e in range(1, inner):
            got_y[i, d, e] = push(
                piece(i, d, 0), piece(i, d, 0), y_peer(e),
                ys.at[d * inner + e, i], yr.at[d * inner + e, i])
        spread(i, d, 0)

    def pass_y(i, d):
        for e in range(1, inner):
            got_y[i, d, e].wait_recv()
            spread(i, d, e)

    def pass_x(d, e):
        for f in range(1, groups):
            got_x[d, e, f].wait_recv()
            at = (d * inner + e) * groups + f
            got_p.append(push(piece(0, d, e, f), piece(0, d, e, f), partner, hs.at[at], hr.at[at]))

    def job(f, *args):
        return functools.partial(f, *args)

    jobs = [job(pass_z, 0, d) for d in turns]
    jobs.insert(1, job(pass_y, 0, 0))
    jobs.append(job(pass_y, 1, 0))
    for d in turns:
        jobs += [job(pass_y, 0, d), job(pass_x, d, 0)]
        if d == turns[0]:
            jobs += [job(pass_x, 0, e) for e in range(1, inner)]
        jobs.append(job(pass_z, 1, d))
    for d in turns:
        jobs += [job(pass_x, d, e) for e in range(1, inner)] + [job(pass_y, 1, d)]

    late = chunks // 2 - 1
    slots = chunks - late + heads_kv + 1
    ran = [0, 0]

    def forward():
        ran[0] += 1
        while ran[1] < len(jobs) * ran[0] // slots:
            jobs[ran[1]]()
            ran[1] += 1

    for c in range(chunks):
        for copy in loads[c]:
            copy.wait()
        for part, w in enumerate((wk, wv)):
            cols = slice(part * width, (part + 1) * width)
            term = jnp.dot(img[c], w[c], preferred_element_type=jnp.float32)
            if c == 0:
                acc[:, cols] = term
            else:
                acc[:, cols] += term
        if c >= late:
            forward()
    vals[...] = acc[:, width:].astype(jnp.bfloat16).reshape(tokens, here, width)
    forward()
    g = gain[...]
    for k in range(heads_kv):
        cols = slice(k * head, (k + 1) * head)
        x = acc[:, cols]
        scale = lax.rsqrt(jnp.mean(x * x, axis=-1, keepdims=True) + 1e-06)
        keys[:, :, cols] = (x * scale * g).astype(jnp.bfloat16).reshape(tokens, here, head)
        forward()

    for copy in local:
        copy.wait()
    for copy in got_p:
        copy.wait_recv()

    id_row = ids[...]
    requests = id_row.shape[1]
    row_at = lax.broadcasted_iota(jnp.int32, (here, requests), 0) + side * here
    col_at = lax.broadcasted_iota(jnp.int32, (here, requests), 1)
    id_col = jnp.sum(jnp.where(row_at == col_at, id_row, 0), axis=1, keepdims=True)
    low = 0.0
    for q in range(2 * groups):
        part = hid[q // groups, :, q % groups * quarter:(q % groups + 1) * quarter]
        low += lax.dot_general(part, all_down[q], NT, preferred_element_type=jnp.float32)
    lane = lax.broadcasted_iota(jnp.int32, low.shape, 1)
    owned = (lane >= id_col * rank) & (lane < id_col * rank + rank)
    low = jnp.where(owned, low, 0.0).astype(jnp.bfloat16)
    queries = []
    for s in range(2):
        delta = jnp.dot(low, all_up[s], preferred_element_type=jnp.float32).astype(jnp.bfloat16)
        queries.append(
            (bas[s].astype(jnp.float32) + delta.astype(jnp.float32)).astype(jnp.bfloat16))
    queries = jnp.concatenate(queries, axis=1)

    eye = lax.broadcasted_iota(jnp.int32, (here, here), 0) == lax.broadcasted_iota(
        jnp.int32, (here, here), 1)
    used_col = jnp.sum(jnp.where(eye, used[...], 0), axis=1, keepdims=True)
    nb = REQUEST_BLOCK
    shape = (group * nb, tokens * nb)
    r_at = lax.broadcasted_iota(jnp.int32, shape, 0)
    c_at = lax.broadcasted_iota(jnp.int32, shape, 1)
    same = (r_at & (nb - 1)) == (c_at & (nb - 1))
    to_exp2 = math.log2(math.e) / math.sqrt(head)
    for b in range(here // nb):
        rs = slice(b * nb, (b + 1) * nb)
        limit = jnp.concatenate([used_col[rs]] * group, axis=0) * (TILE_TOKENS * nb)
        mask = same & (c_at < limit)
        weighed = []
        for k in range(heads_kv):
            cols = slice(k * head, (k + 1) * head)
            kb = keys[:, rs, cols].reshape(tokens * nb, head)
            q = jnp.concatenate(
                [queries[rs, (k * group + i) * head:(k * group + i + 1) * head]
                 for i in range(group)], axis=0)
            weighed.append(lax.dot_general(q, kb, NT, preferred_element_type=jnp.float32))
        weighed = [jnp.where(mask, scores, -1e30) for scores in weighed]
        peaks = [jnp.max(scores, axis=1, keepdims=True) for scores in weighed]
        weighed = [jnp.exp2((scores - peak) * to_exp2) for scores, peak in zip(weighed, peaks)]
        totals = [1.0 / jnp.sum(weights, axis=1, keepdims=True) for weights in weighed]
        for k in range(heads_kv):
            vb = vals[:, rs, k * head:(k + 1) * head].reshape(tokens * nb, head)
            mixed = jnp.dot(
                weighed[k].astype(jnp.bfloat16), vb, preferred_element_type=jnp.float32)
            mixed = (mixed * totals[k]).astype(jnp.bfloat16)
            for i in range(group):
                out[rs, (k * group + i) * head:(k * group + i + 1) * head] = (
                    mixed[i * nb:(i + 1) * nb])

    for copy in started:
        copy.wait_send()


def on_device(
    images,
    key_projection,
    value_projection,
    key_norm_gain,
    hidden,
    shared_query_base,
    adapter_down_matrix,
    adapter_up_matrix,
    tenant_adapter_index,
    used_tile_count,
):
    here, tokens, model = images.shape
    rows = here * tokens
    width = key_projection.shape[1]
    half_model = hidden.shape[1]
    half_query = shared_query_base.shape[1]
    rank = adapter_down_matrix.shape[2]
    count = lax.axis_size("aa")
    outer, inner = grid_of(count)
    groups = lax.axis_size("ga")
    flat = jnp.transpose(images, (1, 0, 2)).reshape(rows, model)
    down = jnp.transpose(adapter_down_matrix[0])
    depth = model // CHUNKS
    bf16 = jnp.bfloat16
    hbm = pl.BlockSpec(memory_space=pl.ANY)
    vmem = pl.BlockSpec(memory_space=pltpu.VMEM)
    dma = pltpu.SemaphoreType.DMA
    return pl.pallas_call(
        functools.partial(kernel, outer, inner),
        out_shape=jax.ShapeDtypeStruct((here, 2 * half_query), bf16),
        in_specs=[hbm] * 7 + [vmem] * 3,
        out_specs=vmem,
        scratch_shapes=[
            pltpu.VMEM((CHUNKS, rows, depth), bf16),
            pltpu.VMEM((CHUNKS, depth, width), bf16),
            pltpu.VMEM((CHUNKS, depth, width), bf16),
            pltpu.VMEM((rows, 2 * width), jnp.float32),
            pltpu.VMEM((tokens, here, width), bf16),
            pltpu.VMEM((tokens, here, width), bf16),
            pltpu.VMEM((2 * groups, count * rank, half_model // groups), bf16),
            pltpu.VMEM((2, count * rank, half_query), bf16),
            pltpu.VMEM((2, here, half_model), bf16),
            pltpu.VMEM((2, here, half_query), bf16),
            dma((CHUNKS, 3)),
            dma((4 + 2 * groups,)),
            dma((outer, 2)),
            dma((outer, 2)),
            dma((count, 2)),
            dma((count, 2)),
            dma((count, 2)),
            dma((count, 2)),
            dma((2,)),
            dma((2,)),
            dma((count * groups,)),
            dma((count * groups,)),
            dma((count * groups,)),
            dma((count * groups,)),
        ],
        compiler_params=pltpu.CompilerParams(
            collective_id=0, has_side_effects=True, vmem_limit_bytes=60 * 1024 * 1024
        ),
    )(
        flat,
        key_projection,
        value_projection,
        hidden,
        shared_query_base,
        down,
        adapter_up_matrix[0],
        key_norm_gain[None, :],
        tenant_adapter_index.reshape(1, -1),
        used_tile_count[None, :],
    )


def solution(mesh):
    placed = (
        P(("ga", "aa", "ba"), None, None),
        P(),
        P(),
        P(),
        P(("ga", "aa"), "ba"),
        P(("ga", "aa"), "ba"),
        P("aa", None, None),
        P("aa", None, None),
        P(("ga", "aa"), None),
        P(("ga", "aa", "ba")),
    )
    return jax.shard_map(
        on_device,
        mesh=mesh,
        in_specs=placed,
        out_specs=P(("ga", "aa", "ba"), None),
        check_vma=False,
    )
```

```python
import functools
import math

import jax
import jax.numpy as jnp
from jax import lax
from jax.experimental import pallas as pl
from jax.experimental.pallas import tpu as pltpu
from jax.sharding import PartitionSpec as P

TILE_TOKENS = 3
REQUEST_BLOCK = 16
CHUNKS = 8
MESH = pl.DeviceIdType.MESH
NT = (((1,), (1,)), ((), ()))


def grid_of(count):
    inner = max(d for d in range(1, count + 1) if count % d == 0 and d * d <= count)
    return count // inner, inner


def kernel(
    outer, inner, images, wk_hbm, wv_hbm, hidden, base, down, up, gain, ids, used, out,
    img, wk, wv, acc, keys, vals, all_down, all_up, hid, bas,
    in_sem, own_sem, zs, zr, ys, yr, ps, pr, xs, xr, gs, gr, hs, hr,
):
    chunks, rows, depth = img.shape
    _, here, half_model = hid.shape
    half_query = bas.shape[2]
    rank = down.shape[0]
    head = gain.shape[1]
    width = wk.shape[2]
    heads_kv = width // head
    group = 2 * half_query // width
    tokens = rows // here

    me = lax.axis_index("aa")
    side = lax.axis_index("ba")
    groups = lax.axis_size("ga")
    g_at = lax.axis_index("ga")
    quarter = half_model // groups
    other = 1 - side
    z, y = me // inner, lax.rem(me, inner)

    partner = {"ba": other}

    loads = []
    for c in range(chunks):
        cols = pl.ds(c * depth, depth)
        loads.append([
            pltpu.make_async_copy(images.at[:, cols], img.at[c], in_sem.at[c, 0]),
            pltpu.make_async_copy(wk_hbm.at[cols], wk.at[c], in_sem.at[c, 1]),
            pltpu.make_async_copy(wv_hbm.at[cols], wv.at[c], in_sem.at[c, 2]),
        ])

    def halves(ref, s, size):
        start = s * size if isinstance(s, int) else pl.multiple_of(s * size, 128)
        return ref.at[:, pl.ds(start, size)]

    mine = pl.ds(pl.multiple_of(side * here, here), here)
    theirs = pl.ds(pl.multiple_of(other * here, here), here)

    local = [
        pltpu.make_async_copy(hidden.at[mine], hid.at[side], own_sem.at[0]),
        pltpu.make_async_copy(base.at[mine], bas.at[side], own_sem.at[1]),
    ]
    own_rows = pl.ds(pl.multiple_of(me * rank, rank), rank)
    for s in range(2):
        local.append(pltpu.make_async_copy(
            halves(up, s, half_query), all_up.at[s, own_rows], own_sem.at[2 + s]))
    for q in range(2 * groups):
        local.append(pltpu.make_async_copy(
            halves(down, q, quarter), all_down.at[q, own_rows], own_sem.at[4 + q]))

    def z_peer(d):
        if outer & (outer - 1):
            return lax.rem(z + d, outer)
        to, bit = z, 1
        while bit < outer:
            if d & bit:
                to = to + bit - 2 * bit * lax.rem(z // bit, 2)
            bit *= 2
        return to

    def z_from(d):
        return lax.rem(z + (outer - d), outer) if outer & (outer - 1) else z_peer(d)

    def block_rows(d, e):
        b = z_from(d) * inner + lax.rem(y + (inner - e), inner)
        return pl.ds(pl.multiple_of(b * rank, rank), rank)

    def y_peer(e):
        return {"aa": z * inner + lax.rem(y + e, inner)}

    def x_peer(f):
        return {"ga": lax.rem(g_at + f, groups)}

    def quarter_at(f):
        return side * groups + lax.rem(g_at + (groups - f), groups)

    started = []

    def push(src, dst, device, ssem, rsem):
        copy = pltpu.make_async_remote_copy(
            src_ref=src, dst_ref=dst, send_sem=ssem, recv_sem=rsem,
            device_id=device, device_id_type=MESH)
        copy.start()
        started.append(copy)
        return copy

    def piece(i, d, e, f=0):
        r = block_rows(d, e)
        return all_up.at[side, r] if i else all_down.at[quarter_at(f), r]

    own_piece = [piece(0, 0, 0), piece(1, 0, 0)]
    ahead = 3
    barrier = pltpu.get_barrier_semaphore()
    greeted = (
        [{"aa": z_peer(d) * inner + y} for d in range(1, outer)]
        + ([{"aa": z_from(d) * inner + y} for d in range(1, outer)] if outer & (outer - 1) else [])
        + [y_peer(e) for e in range(1, inner)]
        + [x_peer(f) for f in range(1, groups)]
        + [partner]
    )
    for device in greeted:
        pl.semaphore_signal(barrier, inc=1, device_id=device, device_id_type=MESH)
    for copy in local[2:] + local[:2]:
        copy.start()
    for copies in loads[:ahead]:
        for copy in copies:
            copy.start()
    pl.semaphore_wait(barrier, len(greeted))
    for copy in local[2:]:
        copy.wait()

    got_z, got_y, got_x, got_p = {}, {}, {}, []
    turns = list(range(1, outer))
    for i in range(2):
        for d in turns:
            got_z[i, d] = push(
                own_piece[i], piece(i, 0, 0), {"aa": z_peer(d) * inner + y}, zs.at[d, i], zr.at[d, i])
        for e in range(1, inner):
            got_y[i, 0, e] = push(own_piece[i], piece(i, 0, 0), y_peer(e), ys.at[e, i], yr.at[e, i])
    for i, (src, dst) in enumerate(((hidden, hid), (base, bas))):
        got_p.append(push(src.at[theirs], dst.at[side], partner, xs.at[i], xr.at[i]))
    for copies in loads[ahead:]:
        for copy in copies:
            copy.start()

    def spread(i, d, e):
        slot = d * inner + e
        here_piece = piece(i, d, e)
        if i == 0:
            for f in range(1, groups):
                got_x[d, e, f] = push(
                    here_piece, here_piece, x_peer(f),
                    gs.at[slot * groups + f], gr.at[slot * groups + f])
        got_p.append(push(here_piece, here_piece, partner, ps.at[slot, i], pr.at[slot, i]))

    def pass_z(i, d):
        got_z[i, d].wait_recv()
        for e in range(1, inner):
            got_y[i, d, e] = push(
                piece(i, d, 0), piece(i, d, 0), y_peer(e),
                ys.at[d * inner + e, i], yr.at[d * inner + e, i])
        spread(i, d, 0)

    def pass_y(i, d):
        for e in range(1, inner):
            got_y[i, d, e].wait_recv()
            spread(i, d, e)

    def pass_x(d, e):
        for f in range(1, groups):
            got_x[d, e, f].wait_recv()
            at = (d * inner + e) * groups + f
            got_p.append(push(piece(0, d, e, f), piece(0, d, e, f), partner, hs.at[at], hr.at[at]))

    def job(f, *args):
        return functools.partial(f, *args)

    jobs = [job(pass_z, 0, d) for d in turns]
    jobs.insert(1, job(pass_y, 0, 0))
    jobs.append(job(pass_y, 1, 0))
    for d in turns:
        jobs += [job(pass_y, 0, d), job(pass_x, d, 0)]
        if d == turns[0]:
            jobs += [job(pass_x, 0, e) for e in range(1, inner)]
        jobs.append(job(pass_z, 1, d))
    for d in turns:
        jobs += [job(pass_x, d, e) for e in range(1, inner)] + [job(pass_y, 1, d)]

    late = chunks // 2 - 1
    slots = chunks - late + heads_kv + 1
    ran = [0, 0]

    def forward():
        ran[0] += 1
        while ran[1] < len(jobs) * ran[0] // slots:
            jobs[ran[1]]()
            ran[1] += 1

    for c in range(chunks):
        for copy in loads[c]:
            copy.wait()
        for part, w in enumerate((wk, wv)):
            cols = slice(part * width, (part + 1) * width)
            term = jnp.dot(img[c], w[c], preferred_element_type=jnp.float32)
            if c == 0:
                acc[:, cols] = term
            else:
                acc[:, cols] += term
        if c >= late:
            forward()
    vals[...] = acc[:, width:].astype(jnp.bfloat16).reshape(tokens, here, width)
    forward()
    g = gain[...]
    for k in range(heads_kv):
        cols = slice(k * head, (k + 1) * head)
        x = acc[:, cols]
        scale = lax.rsqrt(jnp.mean(x * x, axis=-1, keepdims=True) + 1e-06)
        keys[:, :, cols] = (x * scale * g).astype(jnp.bfloat16).reshape(tokens, here, head)
        forward()

    for copy in local[:2]:
        copy.wait()
    for copy in got_p:
        copy.wait_recv()

    id_row = ids[...]
    requests = id_row.shape[1]
    row_at = lax.broadcasted_iota(jnp.int32, (here, requests), 0) + side * here
    col_at = lax.broadcasted_iota(jnp.int32, (here, requests), 1)
    id_col = jnp.sum(jnp.where(row_at == col_at, id_row, 0), axis=1, keepdims=True)
    low = 0.0
    for q in range(2 * groups):
        part = hid[q // groups, :, q % groups * quarter:(q % groups + 1) * quarter]
        low += lax.dot_general(part, all_down[q], NT, preferred_element_type=jnp.float32)
    lane = lax.broadcasted_iota(jnp.int32, low.shape, 1)
    owned = (lane >= id_col * rank) & (lane < id_col * rank + rank)
    low = jnp.where(owned, low, 0.0).astype(jnp.bfloat16)
    queries = []
    for s in range(2):
        delta = jnp.dot(low, all_up[s], preferred_element_type=jnp.float32).astype(jnp.bfloat16)
        queries.append(
            (bas[s].astype(jnp.float32) + delta.astype(jnp.float32)).astype(jnp.bfloat16))
    queries = jnp.concatenate(queries, axis=1)

    eye = lax.broadcasted_iota(jnp.int32, (here, here), 0) == lax.broadcasted_iota(
        jnp.int32, (here, here), 1)
    used_col = jnp.sum(jnp.where(eye, used[...], 0), axis=1, keepdims=True)
    nb = REQUEST_BLOCK
    shape = (group * nb, tokens * nb)
    r_at = lax.broadcasted_iota(jnp.int32, shape, 0)
    c_at = lax.broadcasted_iota(jnp.int32, shape, 1)
    same = (r_at & (nb - 1)) == (c_at & (nb - 1))
    to_exp2 = math.log2(math.e) / math.sqrt(head)
    for b in range(here // nb):
        rs = slice(b * nb, (b + 1) * nb)
        limit = jnp.concatenate([used_col[rs]] * group, axis=0) * (TILE_TOKENS * nb)
        mask = same & (c_at < limit)
        weighed = []
        for k in range(heads_kv):
            cols = slice(k * head, (k + 1) * head)
            kb = keys[:, rs, cols].reshape(tokens * nb, head)
            q = jnp.concatenate(
                [queries[rs, (k * group + i) * head:(k * group + i + 1) * head]
                 for i in range(group)], axis=0)
            weighed.append(lax.dot_general(q, kb, NT, preferred_element_type=jnp.float32))
        weighed = [jnp.where(mask, scores, -1e30) for scores in weighed]
        peaks = [jnp.max(scores, axis=1, keepdims=True) for scores in weighed]
        weighed = [jnp.exp2((scores - peak) * to_exp2) for scores, peak in zip(weighed, peaks)]
        totals = [1.0 / jnp.sum(weights, axis=1, keepdims=True) for weights in weighed]
        for k in range(heads_kv):
            vb = vals[:, rs, k * head:(k + 1) * head].reshape(tokens * nb, head)
            mixed = jnp.dot(
                weighed[k].astype(jnp.bfloat16), vb, preferred_element_type=jnp.float32)
            mixed = (mixed * totals[k]).astype(jnp.bfloat16)
            for i in range(group):
                out[rs, (k * group + i) * head:(k * group + i + 1) * head] = (
                    mixed[i * nb:(i + 1) * nb])

    for copy in started:
        copy.wait_send()


def on_device(
    images,
    key_projection,
    value_projection,
    key_norm_gain,
    hidden,
    shared_query_base,
    adapter_down_matrix,
    adapter_up_matrix,
    tenant_adapter_index,
    used_tile_count,
):
    here, tokens, model = images.shape
    rows = here * tokens
    width = key_projection.shape[1]
    half_model = hidden.shape[1]
    half_query = shared_query_base.shape[1]
    rank = adapter_down_matrix.shape[2]
    count = lax.axis_size("aa")
    outer, inner = grid_of(count)
    groups = lax.axis_size("ga")
    flat = jnp.transpose(images, (1, 0, 2)).reshape(rows, model)
    down = jnp.transpose(adapter_down_matrix[0])
    depth = model // CHUNKS
    bf16 = jnp.bfloat16
    hbm = pl.BlockSpec(memory_space=pl.ANY)
    vmem = pl.BlockSpec(memory_space=pltpu.VMEM)
    dma = pltpu.SemaphoreType.DMA
    return pl.pallas_call(
        functools.partial(kernel, outer, inner),
        out_shape=jax.ShapeDtypeStruct((here, 2 * half_query), bf16),
        in_specs=[hbm] * 7 + [vmem] * 3,
        out_specs=vmem,
        scratch_shapes=[
            pltpu.VMEM((CHUNKS, rows, depth), bf16),
            pltpu.VMEM((CHUNKS, depth, width), bf16),
            pltpu.VMEM((CHUNKS, depth, width), bf16),
            pltpu.VMEM((rows, 2 * width), jnp.float32),
            pltpu.VMEM((tokens, here, width), bf16),
            pltpu.VMEM((tokens, here, width), bf16),
            pltpu.VMEM((2 * groups, count * rank, half_model // groups), bf16),
            pltpu.VMEM((2, count * rank, half_query), bf16),
            pltpu.VMEM((2, here, half_model), bf16),
            pltpu.VMEM((2, here, half_query), bf16),
            dma((CHUNKS, 3)),
            dma((4 + 2 * groups,)),
            dma((outer, 2)),
            dma((outer, 2)),
            dma((count, 2)),
            dma((count, 2)),
            dma((count, 2)),
            dma((count, 2)),
            dma((2,)),
            dma((2,)),
            dma((count * groups,)),
            dma((count * groups,)),
            dma((count * groups,)),
            dma((count * groups,)),
        ],
        compiler_params=pltpu.CompilerParams(
            collective_id=0, has_side_effects=True, vmem_limit_bytes=60 * 1024 * 1024
        ),
    )(
        flat,
        key_projection,
        value_projection,
        hidden,
        shared_query_base,
        down,
        adapter_up_matrix[0],
        key_norm_gain[None, :],
        tenant_adapter_index.reshape(1, -1),
        used_tile_count[None, :],
    )


def solution(mesh):
    placed = (
        P(("ga", "aa", "ba"), None, None),
        P(),
        P(),
        P(),
        P(("ga", "aa"), "ba"),
        P(("ga", "aa"), "ba"),
        P("aa", None, None),
        P("aa", None, None),
        P(("ga", "aa"), None),
        P(("ga", "aa", "ba")),
    )
    return jax.shard_map(
        on_device,
        mesh=mesh,
        in_specs=placed,
        out_specs=P(("ga", "aa", "ba"), None),
        check_vma=False,
    )
```
